32 devices in a mesh: group: 2 (over x), surf: 16 (over z, y, core).
Axes of the slice: x: 2, y: 2, z: 4, core: 2. Of those that a mesh axis runs over, the one named last changes fastest.
Arguments:
- traces: bfloat16 [4096, 128, 1024], P('surf', 'group'), parts along dimension 1, may hold values from -6 to 6
- operator: bfloat16 [4096, 8, 2, 4096], P('surf'), may hold values from -1 to 1, as said below
- freq_bins: int32 [8], replicated, may hold values from 1 to 511, as said below
- win_lengths: int32 [16], replicated, may hold values from 1 to 96, 1024 in all
- coefficients: float32 [16, 31], replicated, may hold values from -2.5 to 2.5
- neighbour: int32 [4096], P('surf'), may hold values from -2 to 2, as said below
Outputs:
- demultiple: bfloat16 [4096, 128, 1024], P('surf', 'group'), parts along dimension 1
The draws below stay inside these ranges and needn't reach their ends.
There are 2 independent parts, one for each index of `group`. The reference program is written for one: setup_inputs(seed, part) draws one part's arguments, and reference() takes and returns one part's arrays. A program takes and returns all parts, laid end to end along the dimension named above; an argument that names none is the same for every part. Nothing has to cross between parts.
Inputs may be any that keep to these rules, and one draw needn't show every extreme that they name: operator[i, f, c, j] equals operator[j, f, c, i] (reciprocity). `freq_bins`: the 8 bins are distinct. `neighbour`: points of even index take an offset of -2 or -1, points of odd index 1 or 2.
All inputs are finite; a program needn't handle non-finite values.
Results may differ from the reference program's by a relative error of at most 0.004.
Values may be sent and summed in bfloat16 or wider, within the bound.
No kernel may reach another device: no remote copies, remote signals or barrier semaphores. Data moves between devices by JAX's collectives and lax.ppermute only.
A program may use at most 192 MiB of HBM per device.

```python
import math
import jax
import jax.numpy as jnp
import numpy as np
from jax import lax

NPTS = 4096
F = 8
NT = 1024
SHOTS = 64
TAPS = 31
HALO = 2
NWIN = 16


def draw_operator(key, part):
    values = jax.random.uniform(key, (NPTS, F, 2, NPTS), jnp.float32, -1.0, 1.0)
    mirrored = 0.5 * (values + jnp.transpose(values, (3, 1, 2, 0)))
    return (mirrored * (3.0 / NPTS) ** 0.5).astype(jnp.bfloat16)


def draw_freq_bins(key, part):
    return (jax.random.permutation(key, NT // 2 - 1)[:F] + 1).astype(jnp.int32)


def draw_neighbour(key, part):
    reach = jax.random.randint(key, (NPTS,), 1, 3, jnp.int32)
    parity = jnp.arange(NPTS, dtype=jnp.int32) % 2
    return (reach * (2 * parity - 1)).astype(jnp.int32)


def level_of(stream_key, shape, split, smallest, top_value):
    loudness = 1.0
    for dim, blocks in split:
        heights = jax.random.uniform(jax.random.fold_in(jax.random.fold_in(stream_key, 6), dim), (blocks,), jnp.float32, smallest / len(split), top_value / len(split))
        loudness = loudness * jnp.repeat(jnp.exp(heights), shape[dim] // blocks).reshape((-1,) + (1,) * (len(shape) - 1 - dim))
    return loudness


def profile(count, total, most, slope):
    portions = [(1 << 20) // math.isqrt(grade ** slope) + 1 for grade in range(2, count + 1)]
    rest, given = total - most - (count - 1), [1] * (count - 1)
    while rest > 0:
        movable = [i for i in range(count - 1) if given[i] < most]
        pool, left = sum([portions[i] for i in movable]), rest
        for i in movable:
            more = min(most - given[i], max(1, left * portions[i] // pool), rest)
            given[i] = given[i] + more
            rest = rest - more
    return np.array([most] + given)


def ragged(rng, amount, total, most, slope):
    if amount == 2:
        one = jax.random.randint(rng, (), max(1, total - most), min(most, total - 1) + 1)
        return jnp.stack([one, total - one])
    tallies = jnp.asarray(profile(amount, total, most, slope), jnp.int32)
    twos = (amount - 1) // 2
    giver, taker = tallies[1:1 + 2 * twos:2], tallies[2:2 + 2 * twos:2]
    margin = jnp.minimum(giver - 1, most - taker)
    moved = jax.random.randint(jax.random.fold_in(rng, 1), (twos,), 0, 1 << 20) % (margin + 1)
    tallies = tallies.at[1:1 + 2 * twos:2].set(giver - moved).at[2:2 + 2 * twos:2].set(taker + moved)
    return tallies[jax.random.permutation(jax.random.fold_in(rng, 2), amount)]


def gaussian(own_key, shape, spread, bound, shards=(), kind=jnp.bfloat16):
    array = jax.random.normal(own_key, shape, jnp.float32) * spread
    if len(shards) > 0:
        array = level_of(own_key, shape, shards, -0.22, 0.18) * array
    return jnp.clip(array, min=-bound, max=bound).astype(kind)


def setup_inputs(seed: int = 0, part: int = 0) -> dict:
    splits = jax.random.split(jax.random.key(seed), 7)
    own_keys = jax.random.split(jax.random.fold_in(splits[6], part), 7)
    traces = gaussian(own_keys[0], (NPTS, SHOTS, NT), 1.0, 6.0, ((0, 16),))
    operator = draw_operator(jax.random.fold_in(splits[6], 71), part)
    freq_bins = draw_freq_bins(jax.random.fold_in(splits[6], 71), part)
    win_lengths = ragged(splits[3], NWIN, NT, NT * 3 // (2 * NWIN), 0).astype(jnp.int32)
    coefficients = gaussian(splits[4], (NWIN, TAPS), 0.18, 2.5, (), jnp.float32)
    neighbour = draw_neighbour(jax.random.fold_in(splits[6], 71), part)
    return dict(traces=traces, operator=operator, freq_bins=freq_bins, win_lengths=win_lengths, coefficients=coefficients, neighbour=neighbour)


def angle_grid(freq_bins):
    sample_index = jnp.arange(NT, dtype=jnp.int32)
    phases = (sample_index[:, None] * freq_bins[None, :]) % NT
    return (2.0 * math.pi / NT) * phases.astype(jnp.float32)


def matching(multiple_estimate, coefficients, win_lengths):
    half_taps = (TAPS - 1) // 2
    window_ends = jnp.cumsum(win_lengths)
    sample_index = jnp.arange(NT, dtype=jnp.int32)
    window = jnp.sum((window_ends[None, :] <= sample_index[:, None]).astype(jnp.int32), axis=1)
    membership = (window[:, None] == jnp.arange(NWIN, dtype=jnp.int32)[None, :]).astype(jnp.float32)
    per_sample = jnp.dot(membership, coefficients, precision=lax.Precision.HIGHEST)
    padded = jnp.pad(multiple_estimate, ((0, 0), (0, 0), (half_taps, half_taps)))
    summed = jnp.zeros_like(multiple_estimate)
    for lag_index in range(TAPS):
        summed = summed + per_sample[:, lag_index] * padded[:, :, lag_index:lag_index + NT]
    return summed


def reference(traces, operator, freq_bins, win_lengths, coefficients, neighbour):
    angles = angle_grid(freq_bins)
    forward = jnp.stack([jnp.cos(angles), -jnp.sin(angles)], axis=2).reshape(NT, 2 * F).astype(jnp.bfloat16)
    spectra = jnp.dot(traces.reshape(NPTS * SHOTS, NT), forward, preferred_element_type=jnp.float32).astype(jnp.bfloat16)
    spectra = spectra.reshape(NPTS, SHOTS, F, 2).transpose(0, 2, 3, 1)
    dims = (((0,), (0,)), ((), ()))
    frequency_slices = []
    for freq_index in range(F):
        op_real = operator[:, freq_index, 0, :]
        op_imag = operator[:, freq_index, 1, :]
        sp_real = spectra[:, freq_index, 0, :]
        spectrum_imaginary = spectra[:, freq_index, 1, :]
        real_part = lax.dot_general(op_real, sp_real, dims, preferred_element_type=jnp.float32) - lax.dot_general(op_imag, spectrum_imaginary, dims, preferred_element_type=jnp.float32)
        imag_part = lax.dot_general(op_real, spectrum_imaginary, dims, preferred_element_type=jnp.float32) + lax.dot_general(op_imag, sp_real, dims, preferred_element_type=jnp.float32)
        frequency_slices.append(jnp.stack([real_part, imag_part], axis=1))
    predicted_multiples = jnp.stack(frequency_slices, axis=1)
    norm_divisor = (2.0 * F * NT) ** -0.5
    inverse_transform = norm_divisor * jnp.stack([jnp.cos(angles.T), -jnp.sin(angles.T)], axis=1)
    multiple_estimate = jnp.einsum("izwj,zwn->ijn", predicted_multiples, inverse_transform, precision=lax.Precision.HIGHEST)
    blocks = multiple_estimate.reshape(NPTS // 256, 256, SHOTS, NT)
    filtered = lax.map(lambda span_rows: matching(span_rows, coefficients, win_lengths), blocks).reshape(NPTS, SHOTS, NT)
    padded = jnp.pad(filtered, ((HALO, HALO), (0, 0), (0, 0)))
    adapted = filtered
    for offset in range(-HALO, HALO + 1):
        selector = (neighbour == offset).astype(jnp.float32)[:, None, None]
        adapted = adapted + 0.5 * selector * padded[HALO + offset:HALO + offset + NPTS]
    return (traces.astype(jnp.float32) - adapted).astype(jnp.bfloat16)
```

```python
import math

import jax
import jax.numpy as jnp
from jax import lax
from jax.sharding import PartitionSpec as P

TAPS = 31
HALO = 2


def padded_2(x, sides, width):
    for axis, dim in sides:
        size, length = (lax.axis_size(axis), x.shape[dim])
        up = [(i, (i + 1) % size) for i in range(size - 1)]
        down = [(j, i) for i, j in up]
        last = lax.slice_in_dim(x, length - width, length, axis=dim)
        initial = lax.slice_in_dim(x, 0, width, axis=dim)
        before = lax.ppermute(last, axis, up)
        after = lax.ppermute(initial, axis, down)
        x = jnp.concatenate([before, x, after], axis=dim)
    return x


def angle_grid(freq_bins, samples):
    sample_index = jnp.arange(samples, dtype=jnp.int32)
    phases = sample_index[:, None] * freq_bins[None, :] % samples
    return 2.0 * math.pi / samples * phases.astype(jnp.float32)


def combine_complex_parts(products):
    real_part = products[:, :, 0, 0] - products[:, :, 1, 1]
    imag_part = products[:, :, 0, 1] + products[:, :, 1, 0]
    return jnp.stack([real_part, imag_part], axis=2)


def matching(multiple_estimate, coefficients, win_lengths):
    samples = multiple_estimate.shape[2]
    half_taps = (TAPS - 1) // 2
    window_ends = jnp.cumsum(win_lengths)
    sample_index = jnp.arange(samples, dtype=jnp.int32)
    window = jnp.sum((window_ends[None, :] <= sample_index[:, None]).astype(jnp.int32), axis=1)
    membership = (
        window[:, None] == jnp.arange(coefficients.shape[0], dtype=jnp.int32)[None, :]
    ).astype(jnp.float32)
    per_sample = jnp.dot(membership, coefficients, precision=lax.Precision.HIGHEST)
    padded = jnp.pad(multiple_estimate, ((0, 0), (0, 0), (half_taps, half_taps)))
    summed = jnp.zeros_like(multiple_estimate)
    for lag_index in range(TAPS):
        summed = summed + per_sample[:, lag_index] * padded[:, :, lag_index : lag_index + samples]
    return summed


def to_traces(spectral_domain, basis):
    point_count, freq_count, parts_count, shot_count = spectral_domain.shape
    rows = spectral_domain.transpose(0, 3, 1, 2).reshape(
        point_count * shot_count, freq_count * parts_count
    )
    timed = jnp.dot(rows, basis, precision=lax.Precision.HIGHEST)
    return timed.reshape(point_count, shot_count, basis.shape[1])


def neighbour_mix(central, padded, neighbour):
    row_count = central.shape[0]
    summed = central
    for offset in range(-HALO, HALO + 1):
        selector = (
            (neighbour == offset)
            .astype(jnp.float32)
            .reshape((row_count,) + (1,) * (central.ndim - 1))
        )
        summed = summed + 0.5 * selector * padded[HALO + offset : HALO + offset + row_count]
    return summed


def on_device(traces, operator, freq_bins, win_lengths, coefficients, neighbour):
    local_points, shot_count, samples = traces.shape
    freq_count = freq_bins.shape[0]
    angles = angle_grid(freq_bins, samples)
    forward = (
        jnp.stack([jnp.cos(angles), -jnp.sin(angles)], axis=2)
        .reshape(samples, 2 * freq_count)
        .astype(jnp.bfloat16)
    )
    spectra = jnp.dot(
        traces.reshape(local_points * shot_count, samples),
        forward,
        preferred_element_type=jnp.float32,
    ).astype(jnp.bfloat16)
    spectra = spectra.reshape(local_points, shot_count, freq_count, 2).transpose(0, 2, 3, 1)
    gathered = lax.all_gather(spectra, "surf", axis=0, tiled=True)
    products = jnp.einsum("rfac,cfbs->rfabs", operator, gathered, preferred_element_type=jnp.float32)
    predicted_multiples = combine_complex_parts(products)
    norm_divisor = (2.0 * freq_count * samples) ** (-0.5)
    inverse_transform = norm_divisor * jnp.stack([jnp.cos(angles.T), -jnp.sin(angles.T)], axis=1)
    basis = matching(
        inverse_transform.reshape(2 * freq_count, 1, samples), coefficients, win_lengths
    ).reshape(2 * freq_count, samples)
    padded = padded_2(predicted_multiples.astype(jnp.bfloat16), (("surf", 0),), HALO).astype(
        predicted_multiples.dtype
    )
    mixed = neighbour_mix(predicted_multiples, padded, neighbour)
    adapted = to_traces(mixed, basis)
    return (traces.astype(jnp.float32) - adapted).astype(jnp.bfloat16)


def solution(mesh):
    return jax.shard_map(
        on_device,
        mesh=mesh,
        in_specs=(P("surf", "group", None), P("surf", None, None, None), P(), P(), P(), P("surf")),
        out_specs=P("surf", "group", None),
        check_vma=False,
    )
```

```python
import functools
import math

import jax
import jax.numpy as jnp
from jax import lax
from jax.experimental import pallas as pl
from jax.experimental.pallas import tpu as pltpu
from jax.sharding import PartitionSpec as P

TAPS = 31
HALO = 2
LANES = 128


def ring_of(mesh):
    size = mesh.shape["surf"]
    chips = list(range(size // 2))
    row = mesh.devices.reshape(mesh.shape["group"], size)[0]
    try:
        places = [tuple(row[2 * chip].coords) for chip in chips]
    except AttributeError:
        return chips
    low = [min(place[d] for place in places) for d in range(3)]
    span = [max(place[d] for place in places) - low[d] + 1 for d in range(3)]
    dims = [d for d in range(3) if span[d] > 1]
    if len(dims) != 2 or span[dims[0]] * span[dims[1]] != len(chips):
        return chips
    a, b = dims if span[dims[0]] % 2 == 0 else dims[::-1]
    if span[a] % 2 or len(set(places)) != len(chips):
        return chips
    order = []
    for i in range(span[a]):
        across = range(1, span[b])
        order += [(i, j) for j in (across if i % 2 == 0 else reversed(across))]
    order += [(i, 0) for i in reversed(range(span[a]))]
    at = {(place[a] - low[a], place[b] - low[b]): chip for chip, place in zip(chips, places)}
    return [at[place] for place in order]


def spectra_kernel(freq_ref, traces_ref, out_ref, table_ref, turned_ref):
    points, shots, samples = traces_ref.shape
    freqs = out_ref.shape[0]
    parts = 2 * freqs

    @pl.when(pl.program_id(0) == 0)
    def _():
        time = lax.broadcasted_iota(jnp.int32, table_ref.shape, 0)
        lane = lax.broadcasted_iota(jnp.int32, table_ref.shape, 1)
        bins = jnp.zeros(table_ref.shape, jnp.int32)
        for f in range(freqs):
            bins = jnp.where(lane // 2 == f, freq_ref[f], bins)
        product = time * bins
        if samples & (samples - 1) == 0:
            phases = product & (samples - 1)
        else:
            phases = lax.rem(product, samples)
        angles = 2.0 * math.pi / samples * phases.astype(jnp.float32)
        table = jnp.where(lane % 2 == 0, jnp.cos(angles), -jnp.sin(angles))
        table_ref[...] = table.astype(jnp.bfloat16)

    rows = traces_ref[...].reshape(points * shots, samples)
    bands = jnp.dot(rows, table_ref[...], preferred_element_type=jnp.float32)
    together = LANES // shots
    for group in range(points // together):
        turned = bands[group * LANES : (group + 1) * LANES].T[:parts]
        for j in range(together):
            place = (group * together + j) * parts
            turned_ref[place : place + parts] = turned[:, j * shots : (j + 1) * shots]
    for f in range(freqs):
        real = turned_ref[pl.ds(2 * f, points, stride=parts), :]
        imag = turned_ref[pl.ds(2 * f + 1, points, stride=parts), :]
        out_ref[f] = jnp.concatenate([real, imag], axis=1).astype(jnp.bfloat16)


def spectra_of(traces, freq_bins, first, count):
    _, shots, samples = traces.shape
    freqs = freq_bins.shape[0]
    points = 16
    return pl.pallas_call(
        spectra_kernel,
        grid=(count // points,),
        in_specs=[
            pl.BlockSpec(memory_space=pltpu.SMEM),
            pl.BlockSpec((points, shots, samples), lambda i: (first // points + i, 0, 0)),
        ],
        out_specs=pl.BlockSpec((freqs, points, 2 * shots), lambda i: (0, i, 0)),
        out_shape=jax.ShapeDtypeStruct((freqs, count, 2 * shots), jnp.bfloat16),
        scratch_shapes=[
            pltpu.VMEM((samples, LANES), jnp.bfloat16),
            pltpu.VMEM((points * 2 * freqs, shots), jnp.float32),
        ],
        cost_estimate=pl.CostEstimate(
            flops=2 * count * shots * samples * LANES, bytes_accessed=count * shots * samples * 2, transcendentals=0
        ),
        name="spectra",
    )(freq_bins, traces)


def product_kernel(blocks_ref, swap_ref, op_ref, *refs, pairs, carried, final):
    refs = list(refs)
    pieces = [(refs.pop(0), refs.pop(0)) for _ in range(pairs)]
    carry_ref = refs.pop(0) if carried else None
    out_ref = refs.pop(0)
    acc_ref = refs.pop(0) if final else out_ref
    step = pl.program_id(0)
    receivers, freqs, _, width = op_ref.shape

    @pl.when(step == 0)
    def _():
        acc_ref[...] = carry_ref[...] if carried else jnp.zeros_like(acc_ref)

    swap = swap_ref[0] == 1
    for f in range(freqs):
        a, b = pieces[0][0][f], pieces[0][1][f]
        for i in range(1, pairs):
            a = jnp.where(step == i, pieces[i][0][f], a)
            b = jnp.where(step == i, pieces[i][1][f], b)
        both = jnp.concatenate([jnp.where(swap, b, a), jnp.where(swap, a, b)], axis=0)
        lhs = op_ref[:, f].reshape(2 * receivers, width)
        acc_ref[f] += jnp.dot(lhs, both, preferred_element_type=jnp.float32)

    if final:

        @pl.when(step == pl.num_programs(0) - 1)
        def _():
            combine(acc_ref, out_ref, receivers, freqs)


def combine(acc_ref, out_ref, receivers, freqs):
    width = acc_ref.shape[2]
    lane = lax.broadcasted_iota(jnp.int32, (receivers, width), 1)
    for f in range(freqs):
        with_real = acc_ref[f, pl.ds(0, receivers, stride=2), :]
        with_imag = acc_ref[f, pl.ds(1, receivers, stride=2), :]
        turned = pltpu.roll(with_imag, width // 2, 1)
        both = with_real + jnp.where(lane < width // 2, -turned, turned)
        out_ref[pl.ds(f, receivers, stride=freqs), :] = both


def product_cost(receivers, freqs, width, lanes):
    return pl.CostEstimate(
        flops=4 * receivers * freqs * width * lanes, bytes_accessed=4 * receivers * freqs * width, transcendentals=0
    )


def products_with(operator, blocks, swap, pairs, carry, final):
    receivers, freqs, _, _ = operator.shape
    points, lanes = pairs[0][0].shape[1:]
    whole = lambda *_: (0, 0, 0)
    shape = (freqs, 2 * receivers, lanes)
    acc = pl.BlockSpec(shape, whole)
    piece = pl.BlockSpec((freqs, points, lanes), whole)
    flat = [array for pair in pairs for array in pair]
    if final:
        out_shape = jax.ShapeDtypeStruct((receivers * freqs, lanes), jnp.float32)
        out_specs = pl.BlockSpec((receivers * freqs, lanes), lambda *_: (0, 0))
    else:
        out_shape, out_specs = jax.ShapeDtypeStruct(shape, jnp.float32), acc
    return pl.pallas_call(
        functools.partial(product_kernel, pairs=len(pairs), carried=carry is not None, final=final),
        grid_spec=pltpu.PrefetchScalarGridSpec(
            num_scalar_prefetch=2,
            grid=(len(pairs),),
            in_specs=[pl.BlockSpec((receivers, freqs, 2, 2 * points), lambda i, at, _: (0, 0, 0, at[i]))]
            + [piece] * len(flat)
            + ([acc] if carry is not None else []),
            out_specs=out_specs,
            scratch_shapes=[pltpu.VMEM(shape, jnp.float32)] if final else [],
        ),
        out_shape=out_shape,
        input_output_aliases={3 + len(flat): 0} if carry is not None and not final else {},
        cost_estimate=product_cost(receivers, freqs, 2 * points * len(pairs), lanes),
        name="product",
    )(blocks, swap, operator, *flat, *([carry] if carry is not None else []))


def whole_product_kernel(op_ref, spectra_ref, out_ref, acc_ref):
    step = pl.program_id(0)
    receivers, freqs, _, width = op_ref.shape

    @pl.when(step == 0)
    def _():
        acc_ref[...] = jnp.zeros_like(acc_ref)

    for f in range(freqs):
        lhs = op_ref[:, f].reshape(2 * receivers, width)
        acc_ref[f] += jnp.dot(lhs, spectra_ref[f], preferred_element_type=jnp.float32)

    @pl.when(step == pl.num_programs(0) - 1)
    def _():
        combine(acc_ref, out_ref, receivers, freqs)


def whole_product(operator, spectra):
    receivers, freqs, _, sources = operator.shape
    lanes = spectra.shape[2]
    width = 4 * LANES
    return pl.pallas_call(
        whole_product_kernel,
        grid=(sources // width,),
        in_specs=[
            pl.BlockSpec((receivers, freqs, 2, width), lambda i: (0, 0, 0, i)),
            pl.BlockSpec((freqs, width, lanes), lambda i: (0, i, 0)),
        ],
        out_specs=pl.BlockSpec((receivers * freqs, lanes), lambda i: (0, 0)),
        out_shape=jax.ShapeDtypeStruct((receivers * freqs, lanes), jnp.float32),
        scratch_shapes=[pltpu.VMEM((freqs, 2 * receivers, lanes), jnp.float32)],
        cost_estimate=product_cost(receivers, freqs, sources, lanes),
        name="whole_product",
    )(operator, spectra)


def subtract_points(offset_of, pred_ref, shift, base, basis_ref, traces_ref, out_ref):
    points, shots, samples = traces_ref.shape
    lanes = pred_ref.shape[2]
    lane = lax.broadcasted_iota(jnp.int32, pred_ref.shape[1:], 1)
    low = lane < lanes // 2
    columns = []
    for p in range(0, points, 2):
        mixed = []
        for q in (p, p + 1):
            here = pred_ref[base + q + shift]
            there = pred_ref[base + q + shift + offset_of(q)]
            mixed.append(here + 0.5 * there)
        first, second = mixed
        real = jnp.where(low, first, pltpu.roll(second, lanes // 2, 1))
        imag = jnp.where(low, pltpu.roll(first, lanes // 2, 1), second)
        columns.append(jnp.concatenate([real, imag], axis=0))
    rows = jnp.concatenate(columns, axis=1)
    high = rows.astype(jnp.bfloat16)
    rest = (rows - high.astype(jnp.float32)).astype(jnp.bfloat16)
    left = jnp.concatenate([high, rest, high], axis=0)
    adapted = lax.dot_general(left, basis_ref[...], (((0,), (0,)), ((), ())), preferred_element_type=jnp.float32)
    traces = traces_ref[...].reshape(points * shots, samples).astype(jnp.float32)
    out_ref[...] = (traces - adapted).astype(jnp.bfloat16).reshape(points, shots, samples)


def inner_kernel(offset_ref, pred_ref, basis_ref, traces_ref, out_ref):
    points = traces_ref.shape[0]
    base = (pl.program_id(0) + 1) * points
    subtract_points(lambda q: offset_ref[base + q], pred_ref, 0, base, basis_ref, traces_ref, out_ref)


def edge_kernel(offset_ref, pred_ref, before_ref, after_ref, basis_ref, traces_ref, given_ref, out_ref, near_ref):
    points = traces_ref.shape[0]
    receivers = pred_ref.shape[0]
    step = pl.program_id(0)

    @pl.when(step == 0)
    def _():
        near_ref[:HALO] = before_ref[...]
        near_ref[HALO:] = pred_ref[: points + HALO]

    @pl.when(step == 1)
    def _():
        near_ref[: points + HALO] = pred_ref[receivers - points - HALO :]
        near_ref[points + HALO :] = after_ref[...]

    base = step * (receivers - points)
    subtract_points(lambda q: offset_ref[base + q], near_ref, HALO, 0, basis_ref, traces_ref, out_ref)


def subtract(traces, predicted, neighbour, basis):
    receivers, shots, samples = traces.shape
    freqs, lanes = predicted.shape[1:]
    points = 8
    blocks = receivers // points
    smem = pl.BlockSpec(memory_space=pltpu.SMEM)
    vmem = pl.BlockSpec(memory_space=pltpu.VMEM)
    out_shape = jax.ShapeDtypeStruct(traces.shape, traces.dtype)
    cost = lambda n: pl.CostEstimate(
        flops=2 * n * points * shots * samples * 48, bytes_accessed=4 * n * points * shots * samples, transcendentals=0
    )
    inner = pl.BlockSpec((points, shots, samples), lambda i: (i + 1, 0, 0))
    central = pl.pallas_call(
        inner_kernel,
        grid=(blocks - 2,),
        in_specs=[smem, vmem, vmem, inner],
        out_specs=inner,
        out_shape=out_shape,
        cost_estimate=cost(blocks - 2),
        name="inner",
    )(neighbour, predicted, basis, traces)
    size = lax.axis_size("surf")
    up = [(i, i + 1) for i in range(size - 1)]
    before = lax.ppermute(predicted[receivers - HALO :], "surf", up)
    after = lax.ppermute(predicted[:HALO], "surf", [(j, i) for i, j in up])
    edge = pl.BlockSpec((points, shots, samples), lambda i: (i * (blocks - 1), 0, 0))
    return pl.pallas_call(
        edge_kernel,
        grid=(2,),
        in_specs=[smem, vmem, vmem, vmem, vmem, edge, pl.BlockSpec(memory_space=pl.ANY)],
        out_specs=edge,
        out_shape=out_shape,
        scratch_shapes=[pltpu.VMEM((points + 2 * HALO, freqs, lanes), jnp.float32)],
        input_output_aliases={6: 0},
        cost_estimate=cost(2),
        name="edge",
    )(neighbour, predicted, before, after, basis, traces, central)


def matching(series, coefficients, win_lengths):
    samples = series.shape[1]
    half_taps = (TAPS - 1) // 2
    window_ends = jnp.cumsum(win_lengths)
    sample_index = jnp.arange(samples, dtype=jnp.int32)
    window = jnp.sum((window_ends[None, :] <= sample_index[:, None]).astype(jnp.int32), axis=1)
    membership = (
        window[:, None] == jnp.arange(coefficients.shape[0], dtype=jnp.int32)[None, :]
    ).astype(jnp.float32)
    per_sample = jnp.dot(membership, coefficients, precision=lax.Precision.HIGHEST)
    padded = jnp.pad(series, ((0, 0), (half_taps, half_taps)))
    summed = jnp.zeros_like(series)
    for lag_index in range(TAPS):
        summed = summed + per_sample[:, lag_index] * padded[:, lag_index : lag_index + samples]
    return summed


def basis_of(freq_bins, win_lengths, coefficients, samples):
    freqs = freq_bins.shape[0]
    sample_index = jnp.arange(samples, dtype=jnp.int32)
    phases = freq_bins[:, None] * sample_index[None, :] % samples
    angles = 2.0 * math.pi / samples * phases.astype(jnp.float32)
    norm_divisor = (2.0 * freqs * samples) ** (-0.5)
    waves = norm_divisor * jnp.concatenate([jnp.cos(angles), -jnp.sin(angles)], axis=0)
    basis = matching(waves, coefficients, win_lengths)
    high = lax.reduce_precision(basis, 8, 7)
    high16, rest16 = high.astype(jnp.bfloat16), (basis - high).astype(jnp.bfloat16)
    return jnp.concatenate([high16, high16, rest16], axis=0)


def predict_in_ring(ring, operator, own):
    size = lax.axis_size("surf")
    chips = size // 2
    ahead = []
    for i, chip in enumerate(ring):
        ahead.append((2 * chip, 2 * ring[(i + 1) % chips]))
        ahead.append((2 * chip + 1, 2 * ring[(i - 1) % chips] + 1))
    across = [(i, i ^ 1) for i in range(size)]
    step_ring = lambda x: lax.ppermute(x, "surf", ahead)
    step_chip = lambda x: lax.ppermute(x, "surf", across)

    me = lax.axis_index("surf")
    core = me % 2
    order = jnp.asarray(ring, jnp.int32)
    position = jnp.argmax(order == me // 2).astype(jnp.int32)
    away = jnp.where(core == 0, -1, 1)
    chip_at = lambda hops: order[(position + away * hops + chips) % chips]
    same = core.astype(jnp.int32)[None]

    half = chips // 2
    u, w = own, step_chip(own)
    carry = None
    pending = ([chip_at(0)], [(u, w)])
    for k in range(1, half):
        u_next, w_next = step_ring(u), step_ring(w)
        carry = products_with(operator, jnp.stack(pending[0]), same, pending[1], carry, False)
        u, w = u_next, w_next
        v, x = step_chip(u), step_chip(w)
        pending = ([chip_at(k), chip_at(-k)], [(u, w), (x, v)])
    u = step_ring(u)
    carry = products_with(operator, jnp.stack(pending[0]), same, pending[1], carry, False)
    v = step_chip(u)
    return products_with(operator, chip_at(half)[None], same, [(u, v)], carry, True)


def on_device(ring, traces, operator, freq_bins, win_lengths, coefficients, neighbour):
    points, shots, samples = traces.shape
    freqs = freq_bins.shape[0]
    own = spectra_of(traces, freq_bins, 0, points)
    if 2 * points % LANES == 0 and len(ring) % 2 == 0 and len(ring) <= 8:
        predicted = predict_in_ring(ring, operator, own)
    else:
        gathered = lax.all_gather(own, "surf", axis=1, tiled=True)
        predicted = whole_product(operator, gathered)
    predicted = predicted.reshape(points, freqs, 2 * shots)
    basis = basis_of(freq_bins, win_lengths, coefficients, samples)
    return subtract(traces, predicted, neighbour, basis)


def solution(mesh):
    return jax.shard_map(
        functools.partial(on_device, ring_of(mesh)),
        mesh=mesh,
        in_specs=(P("surf", "group", None), P("surf", None, None, None), P(), P(), P(), P("surf")),
        out_specs=P("surf", "group", None),
        check_vma=False,
    )
```
